512 devices in a mesh: blk: 32 (over x_lo, y, core), col: 16 (over x_hi, z).
Axes of the slice: x: 4 (x_hi: 2, x_lo: 2; x = x_hi * 2 + x_lo), y: 8, z: 8, core: 2. Of those that a mesh axis runs over, the one named last changes fastest.
Arguments:
- documents: bfloat16 [24576, 768], P('blk'), may hold values from -6 to 6
- landmarks: bfloat16 [65536, 768], P(('blk', 'col')), may hold values from -6 to 6
- eigen_vectors: bfloat16 [65536, 256], P(('blk', 'col')), may hold values from -6 to 6
- land_degree: float32 [65536], P(('blk', 'col')), may hold values from 0.5 to 8
- eigen_values: float32 [256], replicated, may hold values from 0.005 to 0.05
- tile_mask: int32 [192, 512], P('blk'), may hold values from 0 to 1, as said below
- labels: int32 [24576], P(('blk', 'col')), may hold values from 0 to 999
Outputs:
- embedding: float32 [24576, 256], P(('blk', 'col'))
- centroids: float32 [1000, 256], replicated
The draws below stay inside these ranges and needn't reach their ends.
Inputs may be any that keep to these rules, and one draw needn't show every extreme that they name: `tile_mask`: 1 marks a live tile of 128 documents by 128 landmarks; every document block has at least one live tile.
All inputs are finite; a program needn't handle non-finite values.
Results may differ from the reference program's by a relative error of at most 0.0041.
Values may be sent and summed in bfloat16 or wider, within the bound.
A program may use at most 64 MiB of HBM per device.

```python
import math
import jax
import jax.numpy as jnp
from jax import lax

F = 768
K = 256
C = 1000
BLOCK = 128
ND = 24576
NL = 65536


def draw_tile_mask(key, part):
    doc_rows = ND // BLOCK
    land_cols = NL // BLOCK
    base = jax.random.fold_in(key, 17)
    first, second, third = jax.random.split(base, 3)
    level = jax.random.randint(first, (doc_rows, 1), 0, 6)
    coins = jax.random.randint(second, (doc_rows, land_cols), 0, 64)
    alive = coins < jnp.left_shift(jnp.ones_like(level), level)
    forced = jax.random.randint(third, (doc_rows, 1), 0, land_cols)
    struck = jnp.arange(land_cols, dtype=jnp.int32)[None, :] == forced
    return jnp.logical_or(alive, struck).astype(jnp.int32)


def set_ends(array, rng, low, high):
    longest = array.shape.index(max(array.shape))
    spots = []
    for shift in (0, 1):
        where = [jax.random.randint(jax.random.fold_in(rng, axis), (), 0, length) for axis, length in enumerate(array.shape)]
        where[longest] = (where[longest] + shift) % array.shape[longest]
        spots.append(tuple(where))
    return array.at[spots[0]].set(low).at[spots[1]].set(high)


def levels(stream_key, dims, shards, least, high):
    level, own = 1.0, jax.random.fold_in(stream_key, 6)
    for axis_at, parts in shards:
        heights = jnp.exp(jax.random.uniform(jax.random.fold_in(own, axis_at), (parts,), jnp.float32, least / len(shards), high / len(shards)))
        level = level * jnp.repeat(heights, dims[axis_at] // parts).reshape([-1 if axis == axis_at else 1 for axis in range(len(dims))])
    return level


def bell_draw(rng, extent, width, reach, pieces=(), held_as=jnp.bfloat16):
    level = levels(rng, extent, pieces, -0.22, 0.18) if pieces else 1.0
    values = jax.random.normal(rng, extent, jnp.float32) * width * level
    return jnp.minimum(jnp.maximum(values, -reach), reach).astype(held_as)


def setup_inputs(seed: int = 0) -> dict:
    key_list = jax.random.split(jax.random.key(seed), 8)
    return {
        "documents": bell_draw(key_list[0], (ND, F), 1.0, 6.0, ((0, 32),)),
        "landmarks": bell_draw(key_list[1], (NL, F), 1.0, 6.0, ((0, 512),)),
        "eigen_vectors": bell_draw(key_list[2], (NL, K), 1.0, 6.0, ((0, 512),)),
        "land_degree": jnp.clip(jnp.exp(math.log(8.0) - 2.7725887 * jax.random.uniform(key_list[3], (NL,), jnp.float32) ** levels(key_list[3], (NL,), ((0, 512),), -0.2, 0.2)), 0.5, 8.0),
        "eigen_values": jnp.clip(jnp.exp(jax.random.uniform(key_list[4], (K,), jnp.float32, math.log(0.005), math.log(0.05))), 0.005, 0.05),
        "tile_mask": draw_tile_mask(jax.random.fold_in(key_list[7], 71), 0),
        "labels": set_ends(jax.random.randint(key_list[6], (ND,), 0, C), jax.random.fold_in(key_list[6], 1), 0, C - 1).astype(jnp.int32),
    }


def reference(documents, landmarks, eigen_vectors, land_degree, eigen_values, tile_mask, labels):
    inverse_width = 4.0 / F
    scaled = (eigen_vectors.astype(jnp.float32) * lax.rsqrt(land_degree)[:, None] / eigen_values[None, :]).astype(jnp.bfloat16)
    land_blocks = landmarks.reshape(NL // BLOCK, BLOCK, F)
    vector_blocks = scaled.reshape(NL // BLOCK, BLOCK, K)
    land_square = lax.optimization_barrier(jnp.sum(jnp.square(landmarks.astype(jnp.float32)), 1)).reshape(NL // BLOCK, BLOCK)
    doc_blocks = documents.reshape(ND // BLOCK, BLOCK, F)

    def one_block(item):
        doc_block, live_row = item
        doc_square = lax.optimization_barrier(jnp.sum(jnp.square(doc_block.astype(jnp.float32)), 1))

        def step(carry, index):

            def absorb(state):
                land_block = lax.dynamic_index_in_dim(land_blocks, index, 0, keepdims=False)
                vector_block = lax.dynamic_index_in_dim(vector_blocks, index, 0, keepdims=False)
                square_block = lax.dynamic_index_in_dim(land_square, index, 0, keepdims=False)
                products = jnp.einsum('df,lf->dl', doc_block, land_block, preferred_element_type=jnp.float32)
                weights = jnp.exp(inverse_width * (2.0 * products - doc_square[:, None] - square_block[None, :]))
                total = state[0] + jnp.dot(weights.astype(jnp.bfloat16), vector_block, preferred_element_type=jnp.float32)
                return (total, state[1] + lax.optimization_barrier(jnp.sum(weights, 1)))
            live_flag = lax.dynamic_index_in_dim(live_row, index, 0, keepdims=False)
            return (lax.cond(live_flag > 0, absorb, lambda state: state, carry), None)
        initial = (jnp.zeros((BLOCK, K), jnp.float32), jnp.zeros((BLOCK,), jnp.float32))
        result, unused = lax.scan(step, initial, jnp.arange(NL // BLOCK, dtype=jnp.int32))
        return result
    projection, degree = lax.map(one_block, (doc_blocks, tile_mask))
    projection = projection.reshape(ND, K)
    degree = degree.reshape(ND)
    embedding = projection * lax.rsqrt(degree)[:, None]
    unit_rows = embedding * lax.rsqrt(lax.optimization_barrier(jnp.sum(jnp.square(embedding), 1, keepdims=True)) + 1e-06)
    centroids = jax.ops.segment_sum(unit_rows, labels, num_segments=C)
    return (embedding, centroids)
```

```python
import math
import jax
import jax.numpy as jnp
from jax import lax
from jax.experimental import pallas as pl
from jax.experimental.pallas import tpu as pltpu
from jax.sharding import PartitionSpec as P

C = 1000
BLOCK = 128
MESH = pl.DeviceIdType.MESH
F32, BF16 = jnp.float32, jnp.bfloat16
NX, NY, NZ = 4, 8, 8
HALF = 64
DEAD = -1e30


def wrap(value, n):
    return lax.rem(value + n, n)


def device(x, y, core, z):
    x_high = lax.div(x, 2)
    x_low = x - 2 * x_high
    return {"blk": x_low * 16 + y * 2 + core, "col": x_high * 8 + z}


def rows_dot(a, b):
    return lax.dot_general(a, b, (((1,), (1,)), ((), ())), preferred_element_type=F32)


def split_rows_dot(ones, value, pieces):
    total, left = None, value
    for piece in range(pieces):
        part = left.astype(BF16)
        left = left - part.astype(F32)
        term = rows_dot(ones, part)
        total = term if total is None else total + term
    return total


def diagonal(row, n):
    square = jnp.broadcast_to(row, (n, n))
    down = lax.broadcasted_iota(jnp.int32, (n, n), 0)
    across = lax.broadcasted_iota(jnp.int32, (n, n), 1)
    return jnp.sum(jnp.where(down == across, square, 0.0), axis=1, keepdims=True)


class Sends:
    def __init__(self, sems):
        self.sems, self.used, self.open = sems, 0, []

    def start(self, src, dst, recv, to):
        copy = pltpu.make_async_remote_copy(
            src_ref=src, dst_ref=dst, send_sem=self.sems.at[self.used], recv_sem=recv,
            device_id=to, device_id_type=MESH,
        )
        self.used += 1
        copy.start()
        self.open.append(copy)

    def finish(self):
        for copy in self.open:
            copy.wait_send()


def arrived(ref, sems, index, frm):
    pltpu.make_async_remote_copy(
        src_ref=ref, dst_ref=ref, send_sem=sems.at[index], recv_sem=sems.at[index],
        device_id=frm, device_id_type=MESH,
    ).wait_recv()


def kernel(
    docs_ref, land_ref, vec_ref, ldeg_ref, eval_ref, mask_ref, label_ref,
    emb_ref, cent_ref,
    L, D, DC, M, KEEP, BIAS, PR, DG, PIN, DIN, SP, RP, SD, RD, G, SY, RY, RZ, W,
    local_sem, send_sem, y_sem, x_sem, core_sem, col_sem, cold_sem, g_sem, ry_sem, rz_sem, wy_sem, wx_sem, wc_sem,
):
    blk, col = lax.axis_index("blk"), lax.axis_index("col")
    x_low = lax.div(blk, 16)
    core = lax.rem(blk, 2)
    y = lax.rem(lax.div(blk, 2), 8)
    x_high = lax.div(col, 8)
    z = lax.rem(col, 8)
    x = x_high * 2 + x_low
    other = 1 - core
    features = docs_ref.shape[1]
    scale = 4.0 / features * math.log2(math.e)

    partner = device(x, y, other, z)
    up, down = device(x, wrap(y + 1, NY), core, z), device(x, wrap(y - 1, NY), core, z)
    right, left = device(wrap(x + 1, NX), y, core, z), device(wrap(x - 1, NX), y, core, z)

    own_docs = pltpu.make_async_copy(docs_ref, D.at[0], local_sem)
    own_docs.start()

    barrier = pltpu.get_barrier_semaphore()
    near = [partner]
    for d in range(1, NX):
        near += [device(wrap(x + d, NX), y, core, z), device(wrap(x + d, NX), y, other, z)]
    for d in range(1, NY):
        near.append(device(x, wrap(y + d, NY), core, z))
    for d in range(1, 16):
        near.append({"blk": blk, "col": lax.rem(col + d, 16)})
    near = near[:3] + near[4:]
    for peer in near:
        pl.semaphore_signal(barrier, inc=1, device_id=peer, device_id_type=MESH)

    inverse_root = diagonal(lax.rsqrt(ldeg_ref[...]), BLOCK)
    scaled = vec_ref[...].astype(F32) * inverse_root / eval_ref[...]
    L[y, 0:BLOCK, 0:features] = land_ref[...]
    L[y, 0:BLOCK, features:] = scaled.astype(BF16)
    M[0] = jnp.zeros(M.shape[1:], F32)
    M[0, 0:6, :] = mask_ref[...].astype(F32)
    pl.semaphore_wait(barrier, len(near))

    sends = Sends(send_sem)
    A, B = pl.ds(0, HALF), pl.ds(HALF, HALF)
    KINDS = {("A", 1): 0, ("B", 1): 1, ("A", -1): 2, ("B", -1): 3}

    def along_y(half, way, step):
        block = wrap(y - way * (step - 1), NY)
        piece = L.at[block, A if half == "A" else B]
        sends.start(piece, piece, y_sem.at[KINDS[half, way], step - 1], up if way == 1 else down)

    def along_x(half, offset):
        block = wrap(y + offset, NY)
        if half == "A":
            sends.start(L.at[block, A], L.at[block, pl.ds(2 * HALF, HALF)], x_sem.at[0, offset % NY], right)
        else:
            sends.start(L.at[block, B], L.at[block, pl.ds(3 * HALF, HALF)], x_sem.at[1, offset % NY], left)

    def from_y(half, way, step):
        block = wrap(y - way * step, NY)
        piece = L.at[block, A if half == "A" else B]
        arrived(piece, y_sem.at[KINDS[half, way]], step - 1, down if way == 1 else up)

    def from_x(offset):
        block = wrap(y + offset, NY)
        arrived(L.at[block, pl.ds(2 * HALF, HALF)], x_sem.at[0], offset % NY, left)
        arrived(L.at[block, pl.ds(3 * HALF, HALF)], x_sem.at[1], offset % NY, right)

    along_y("A", 1, 1)
    along_y("B", -1, 1)
    along_x("A", 0)
    along_x("B", 0)
    along_y("B", 1, 1)
    along_y("A", -1, 1)
    sends.start(M.at[0], M.at[1], core_sem.at[0], partner)
    own_docs.wait()
    sends.start(D.at[0], D.at[1], core_sem.at[1], partner)

    PR[...] = jnp.zeros(PR.shape, F32)
    DG[...] = jnp.zeros(DG.shape, F32)
    arrived(M.at[1], core_sem, 0, partner)
    live = M[...].reshape(16, M.shape[2])
    tiles = lax.broadcasted_iota(jnp.int32, live.shape, 1)
    segment = lax.div(lax.broadcasted_iota(jnp.int32, (16, 4 * HALF), 1), HALF)

    def tile_of(source_x, block):
        high = lax.div(source_x, 2)
        return (source_x - 2 * high) * 256 + block * 32 + core * 16 + high * 8 + z

    for block in range(NY):
        cols = [
            jnp.sum(jnp.where(tiles == tile_of(source, block), live, 0.0), axis=1, keepdims=True)
            for source in (x, wrap(x - 1, NX), wrap(x + 1, NX))
        ]
        keep = jnp.where(segment < 2, cols[0], jnp.where(segment < 3, cols[1], cols[2]))
        KEEP[block] = jnp.where(keep > 0.0, 0.0, DEAD)

    arrived(D.at[1], core_sem, 1, partner)

    def squares(chunk, carry):
        who, at = lax.div(chunk, 2), lax.rem(chunk, 2) * 384
        rows = D[who, pl.ds(pl.multiple_of(at, 384), 384), :].astype(F32)
        total = jnp.sum(rows * rows, axis=1, keepdims=True) * (-scale)
        DC[who, pl.ds(pl.multiple_of(at, 384), 384), :] = jnp.broadcast_to(total, (384, 128))
        return carry

    lax.fori_loop(0, 4, squares, 0)
    ones = jnp.ones((8, features), BF16)

    def prepare(offset):
        block = wrap(y + offset, NY)
        values = L[block, :, 0:features].astype(F32)
        norms = split_rows_dot(ones, values * values, 2)
        BIAS[...] = KEEP[block] - scale * norms[0:1, :]

    def multiply(offset, who, part):
        block = wrap(y + offset, NY)
        at = pl.multiple_of(part * 384, 384)
        docs = D[who, pl.ds(at, 384), :]
        products = rows_dot(docs, L[block, :, 0:features])
        shift = DC[who, pl.ds(at, 384), :]
        shift = jnp.concatenate([shift, shift], axis=1)
        bias = jnp.concatenate(
            [jnp.broadcast_to(BIAS[pl.ds(who * 8 + part * 3 + i, 1), :], (128, 256)) for i in range(3)], axis=0
        )
        weights = jnp.exp2(products * (2.0 * scale) + shift + bias)
        groups = pl.ds(part * 8, 8)
        DG[who, groups] += (weights[:, 0:128] + weights[:, 128:256]).reshape(8, 48, 128)
        total = jnp.dot(weights.astype(BF16), L[block, :, features:], preferred_element_type=F32)
        PR[who, groups] += total.reshape(8, 48, 256)

    def batch(offset):
        from_x(offset)
        prepare(offset)

        def part(index, carry):
            multiply(offset, 1 - lax.div(index, 2), lax.rem(index, 2))
            return carry

        lax.fori_loop(0, 4, part, 0)

    for step in range(1, 5):
        from_y("A", 1, step)
        if step < 4:
            along_y("A", 1, step + 1)
        along_x("A", -step)
        from_y("B", -1, step)
        if step < 4:
            along_y("B", -1, step + 1)
        along_x("B", step)
        batch(-(step - 1))
        if step < 4:
            from_y("B", 1, step)
            if step < 3:
                along_y("B", 1, step + 1)
            along_x("B", -step)
            from_y("A", -1, step)
            if step < 3:
                along_y("A", -1, step + 1)
            along_x("A", step)
        if step > 1:
            batch(step - 1)

    from_x(4)
    prepare(4)
    for who in (1, 0):
        def part(index, carry, who=who):
            multiply(4, who, index)
            return carry

        lax.fori_loop(0, 2, part, 0)
        if who == 1:
            sends.start(PR.at[1], PIN, core_sem.at[2], partner)
            sends.start(DG.at[1], DIN, core_sem.at[3], partner)

    arrived(PIN, core_sem, 2, partner)
    arrived(DIN, core_sem, 3, partner)
    ones = jnp.ones((8, 128), BF16)

    def degrees(at):
        return split_rows_dot(ones, DG[0, at] + DIN[at], 3)

    for d in range(1, 16):
        to = lax.rem(col + d, 16)
        owner = {"blk": blk, "col": to}
        SP[to] = (PR[0, to] + PIN[to]).astype(BF16)
        SD[to] = jnp.zeros((8, 128), F32)
        SD[to, :, 0:48] = degrees(to)
        sends.start(SP.at[to], RP.at[col], col_sem.at[d], owner)
        sends.start(SD.at[to], RD.at[col], cold_sem.at[d], owner)
    projection = PR[0, col] + PIN[col]
    degree = degrees(col)
    for d in range(1, 16):
        frm = lax.rem(col - d + 16, 16)
        owner = {"blk": blk, "col": frm}
        arrived(RP.at[frm], col_sem, d, owner)
        arrived(RD.at[frm], cold_sem, d, owner)
        projection = projection + RP[frm].astype(F32)
        degree = degree + RD[frm, :, 0:48]
    embedding = projection * lax.rsqrt(diagonal(degree[0:1, :], 48))
    emb_ref[...] = embedding
    unit = embedding * lax.rsqrt(jnp.sum(embedding * embedding, axis=1, keepdims=True) + 1e-6)

    mine = x * 2 + core
    label = label_ref[...]
    high = lax.div(label, 32)
    low = label - 32 * high
    two = lax.broadcasted_iota(jnp.int32, (16, 48), 0)
    coded = jnp.where(two == 0, jnp.broadcast_to(high, (16, 48)), jnp.broadcast_to(low, (16, 48)))
    G[mine, 0:48, :] = unit.astype(BF16)
    G[mine, 48:64, :] = jnp.zeros((16, 256), BF16)
    G[mine, 48:64, 0:48] = coded.astype(F32).astype(BF16)
    group = [(d, c) for d in range(NX) for c in range(2) if (d, c) != (0, 0)]
    for index, (d, c) in enumerate(group):
        other_core = core if c == 0 else other
        to = device(wrap(x + d, NX), y, other_core, z)
        sends.start(G.at[mine], G.at[mine], g_sem.at[index], to)
    for index, (d, c) in enumerate(group):
        other_core = core if c == 0 else other
        from_where = wrap(x - d, NX)
        slot = from_where * 2 + other_core
        arrived(G.at[slot], g_sem, index, device(from_where, y, other_core, z))
    clusters = (lax.broadcasted_iota(jnp.int32, (128, 48), 0) + mine * 128).astype(F32)
    sums = jnp.zeros((128, 256), F32)
    for source in range(8):
        code = G[source, 48:64, 0:48].astype(F32)
        which = code[0:1, :] * 32.0 + code[1:2, :]
        hot = jnp.where(clusters == which, 1.0, 0.0).astype(BF16)
        sums = sums + jnp.dot(hot, G[source, 0:48, :], preferred_element_type=F32)
    SY[...] = sums.reshape(8, 16, 256)

    for d in range(1, NY):
        to = wrap(y + d, NY)
        sends.start(SY.at[to], RY.at[y], ry_sem.at[d], device(x, to, core, z))
    RY[y] = SY[y]
    for d in range(1, NY):
        frm = wrap(y - d, NY)
        arrived(RY.at[frm], ry_sem, d, device(x, frm, core, z))
    total = RY[0]
    for source in range(1, NY):
        total = total + RY[source]
    RZ[z] = total

    for d in range(1, NZ):
        sends.start(RZ.at[z], RZ.at[z], rz_sem.at[d], device(x, y, core, wrap(z + d, NZ)))
    for d in range(1, NZ):
        frm = wrap(z - d, NZ)
        arrived(RZ.at[frm], rz_sem, d, device(x, y, core, frm))
    total = RZ[0]
    for source in range(1, NZ):
        total = total + RZ[source]
    W[mine, y] = total.astype(BF16)

    for d in range(1, NY):
        sends.start(W.at[mine, y], W.at[mine, y], wy_sem.at[d], device(x, wrap(y + d, NY), core, z))
    for d in range(1, NY):
        frm = wrap(y - d, NY)
        arrived(W.at[mine, frm], wy_sem, d, device(x, frm, core, z))
    for d in range(1, NX):
        sends.start(W.at[mine], W.at[mine], wx_sem.at[d], device(wrap(x + d, NX), y, core, z))
    sends.start(W.at[mine], W.at[mine], wc_sem.at[0], partner)
    for d in range(1, NX):
        frm = wrap(x - d, NX)
        slot = frm * 2 + core
        arrived(W.at[slot], wx_sem, d, device(frm, y, core, z))
        sends.start(W.at[slot], W.at[slot], wc_sem.at[d], partner)
    for d in range(NX):
        frm = wrap(x - d, NX)
        arrived(W.at[frm * 2 + other], wc_sem, d, partner)
    cent_ref[...] = W[...].reshape(1024, 256)
    sends.finish()


def body(documents, landmarks, eigen_vectors, land_degree, eigen_values, tile_mask, labels):
    rows, features = documents.shape
    k = eigen_vectors.shape[1]
    dma = pltpu.SemaphoreType.DMA
    vmem = pl.BlockSpec(memory_space=pltpu.VMEM)
    embedding, centroids = pl.pallas_call(
        kernel,
        out_shape=(jax.ShapeDtypeStruct((48, k), F32), jax.ShapeDtypeStruct((1024, k), BF16)),
        in_specs=[pl.BlockSpec(memory_space=pl.ANY)] + [vmem] * 6,
        out_specs=(vmem, vmem),
        scratch_shapes=[
            pltpu.VMEM((NY, 4 * HALF, features + k), BF16),
            pltpu.VMEM((2, rows, features), BF16),
            pltpu.VMEM((2, rows, 128), F32),
            pltpu.VMEM((2, 8, 512), F32),
            pltpu.VMEM((NY, 16, 4 * HALF), F32),
            pltpu.VMEM((16, 4 * HALF), F32),
            pltpu.VMEM((2, 16, 48, k), F32),
            pltpu.VMEM((2, 16, 48, 128), F32),
            pltpu.VMEM((16, 48, k), F32),
            pltpu.VMEM((16, 48, 128), F32),
            pltpu.VMEM((16, 48, k), BF16),
            pltpu.VMEM((16, 48, k), BF16),
            pltpu.VMEM((16, 8, 128), F32),
            pltpu.VMEM((16, 8, 128), F32),
            pltpu.VMEM((8, 64, k), BF16),
            pltpu.VMEM((8, 16, k), F32),
            pltpu.VMEM((8, 16, k), F32),
            pltpu.VMEM((8, 16, k), F32),
            pltpu.VMEM((8, 8, 16, k), BF16),
            dma(()),
            dma((128,)),
            dma((4, 4)),
            dma((2, 8)),
            dma((4,)),
            dma((16,)),
            dma((16,)),
            dma((8,)),
            dma((8,)),
            dma((8,)),
            dma((8,)),
            dma((4,)),
            dma((4,)),
        ],
        compiler_params=pltpu.CompilerParams(collective_id=0, has_side_effects=True),
        name="nystrom",
    )(
        documents, landmarks, eigen_vectors, land_degree[None, :], eigen_values[None, :], tile_mask, labels[None, :]
    )
    return embedding, centroids[:C].astype(F32)


def solution(mesh):
    placed = (
        P("blk", None),
        P(("blk", "col"), None),
        P(("blk", "col"), None),
        P(("blk", "col")),
        P(),
        P("blk", None),
        P(("blk", "col")),
    )
    return jax.shard_map(
        body, mesh=mesh, in_specs=placed, out_specs=(P(("blk", "col"), None), P()), check_vma=False
    )
```

```python
import math
import jax
import jax.numpy as jnp
from jax import lax
from jax.experimental import pallas as pl
from jax.experimental.pallas import tpu as pltpu
from jax.sharding import PartitionSpec as P

C = 1000
BLOCK = 128
MESH = pl.DeviceIdType.MESH
F32, BF16 = jnp.float32, jnp.bfloat16
NX, NY, NZ = 4, 8, 8
HALF = 64
DEAD = -1e30


def wrap(value, n):
    return lax.rem(value + n, n)


def device(x, y, core, z):
    x_high = lax.div(x, 2)
    x_low = x - 2 * x_high
    return {"blk": x_low * 16 + y * 2 + core, "col": x_high * 8 + z}


def rows_dot(a, b):
    return lax.dot_general(a, b, (((1,), (1,)), ((), ())), preferred_element_type=F32)


def split_rows_dot(ones, value, pieces):
    total, left = None, value
    for piece in range(pieces):
        part = left.astype(BF16)
        left = left - part.astype(F32)
        term = rows_dot(ones, part)
        total = term if total is None else total + term
    return total


def diagonal(row, n):
    square = jnp.broadcast_to(row, (n, n))
    down = lax.broadcasted_iota(jnp.int32, (n, n), 0)
    across = lax.broadcasted_iota(jnp.int32, (n, n), 1)
    return jnp.sum(jnp.where(down == across, square, 0.0), axis=1, keepdims=True)


class Sends:
    def __init__(self, sems):
        self.sems, self.used, self.open = sems, 0, []

    def start(self, src, dst, recv, to):
        copy = pltpu.make_async_remote_copy(
            src_ref=src, dst_ref=dst, send_sem=self.sems.at[self.used], recv_sem=recv,
            device_id=to, device_id_type=MESH,
        )
        self.used += 1
        copy.start()
        self.open.append(copy)

    def finish(self):
        for copy in self.open:
            copy.wait_send()


def arrived(ref, sems, index, frm):
    pltpu.make_async_remote_copy(
        src_ref=ref, dst_ref=ref, send_sem=sems.at[index], recv_sem=sems.at[index],
        device_id=frm, device_id_type=MESH,
    ).wait_recv()


def kernel(
    docs_ref, land_ref, vec_ref, ldeg_ref, eval_ref, mask_ref, label_ref,
    emb_ref, cent_ref,
    L, D, DC, M, KEEP, BIAS, PR, DG, PIN, DIN, SP, RP, SD, RD, LB, G, SY, RY, RZ, W,
    local_sem, send_sem, y_sem, x_sem, core_sem, col_sem, cold_sem, g_sem, ry_sem, rz_sem, wy_sem, wx_sem, wc_sem, l_sem, word,
):
    blk, col = lax.axis_index("blk"), lax.axis_index("col")
    x_low = lax.div(blk, 16)
    core = lax.rem(blk, 2)
    y = lax.rem(lax.div(blk, 2), 8)
    x_high = lax.div(col, 8)
    z = lax.rem(col, 8)
    x = x_high * 2 + x_low
    other = 1 - core
    features = docs_ref.shape[1]
    scale = 4.0 / features * math.log2(math.e)

    partner = device(x, y, other, z)
    up, down = device(x, wrap(y + 1, NY), core, z), device(x, wrap(y - 1, NY), core, z)
    right, left = device(wrap(x + 1, NX), y, core, z), device(wrap(x - 1, NX), y, core, z)

    own_docs = pltpu.make_async_copy(docs_ref, D.at[0], local_sem)
    own_docs.start()

    barrier = pltpu.get_barrier_semaphore()
    front, back = device(x, y, core, wrap(z + 1, NZ)), device(x, y, core, wrap(z - 1, NZ))
    near = [partner, up, down, right, left, front, back]
    for peer in near:
        pl.semaphore_signal(barrier, inc=1, device_id=peer, device_id_type=MESH)

    inverse_root = diagonal(lax.rsqrt(ldeg_ref[...]), BLOCK)
    scaled = vec_ref[...].astype(F32) * inverse_root / eval_ref[...]
    L[y, 0:BLOCK, 0:features] = land_ref[...]
    L[y, 0:BLOCK, features:] = scaled.astype(BF16)
    M[0] = jnp.zeros(M.shape[1:], F32)
    M[0, 0:6, :] = mask_ref[...].astype(F32)
    pl.semaphore_wait(barrier, len(near))

    sends = Sends(send_sem)
    A, B = pl.ds(0, HALF), pl.ds(HALF, HALF)
    KINDS = {("A", 1): 0, ("B", 1): 1, ("A", -1): 2, ("B", -1): 3}

    def along_y(half, way, step):
        block = wrap(y - way * (step - 1), NY)
        piece = L.at[block, A if half == "A" else B]
        sends.start(piece, piece, y_sem.at[KINDS[half, way], step - 1], up if way == 1 else down)

    def along_x(half, offset):
        block = wrap(y + offset, NY)
        if half == "A":
            sends.start(L.at[block, A], L.at[block, pl.ds(2 * HALF, HALF)], x_sem.at[0, offset % NY], right)
        else:
            sends.start(L.at[block, B], L.at[block, pl.ds(3 * HALF, HALF)], x_sem.at[1, offset % NY], left)

    def from_y(half, way, step):
        block = wrap(y - way * step, NY)
        piece = L.at[block, A if half == "A" else B]
        arrived(piece, y_sem.at[KINDS[half, way]], step - 1, down if way == 1 else up)

    def from_x(offset):
        block = wrap(y + offset, NY)
        arrived(L.at[block, pl.ds(2 * HALF, HALF)], x_sem.at[0], offset % NY, left)
        arrived(L.at[block, pl.ds(3 * HALF, HALF)], x_sem.at[1], offset % NY, right)

    along_y("A", 1, 1)
    along_y("B", -1, 1)
    along_x("A", 0)
    along_x("B", 0)
    along_y("B", 1, 1)
    along_y("A", -1, 1)
    sends.start(M.at[0], M.at[1], core_sem.at[0], partner)
    own_docs.wait()
    sends.start(D.at[0], D.at[1], core_sem.at[1], partner)

    PR[...] = jnp.zeros(PR.shape, F32)
    DG[...] = jnp.zeros(DG.shape, F32)
    arrived(M.at[1], core_sem, 0, partner)
    live = M[...].reshape(16, M.shape[2])
    tiles = lax.broadcasted_iota(jnp.int32, live.shape, 1)
    segment = lax.div(lax.broadcasted_iota(jnp.int32, (16, 4 * HALF), 1), HALF)

    def tile_of(source_x, block):
        high = lax.div(source_x, 2)
        return (source_x - 2 * high) * 256 + block * 32 + core * 16 + high * 8 + z

    for block in range(NY):
        cols = [
            jnp.sum(jnp.where(tiles == tile_of(source, block), live, 0.0), axis=1, keepdims=True)
            for source in (x, wrap(x - 1, NX), wrap(x + 1, NX))
        ]
        keep = jnp.where(segment < 2, cols[0], jnp.where(segment < 3, cols[1], cols[2]))
        KEEP[block] = jnp.where(keep > 0.0, 0.0, DEAD)

    arrived(D.at[1], core_sem, 1, partner)

    def squares(chunk, carry):
        who, at = lax.div(chunk, 2), lax.rem(chunk, 2) * 384
        rows = D[who, pl.ds(pl.multiple_of(at, 384), 384), :].astype(F32)
        total = jnp.sum(rows * rows, axis=1, keepdims=True) * (-scale)
        DC[who, pl.ds(pl.multiple_of(at, 384), 384), :] = jnp.broadcast_to(total, (384, 128))
        return carry

    lax.fori_loop(0, 4, squares, 0)
    ones = jnp.ones((8, features), BF16)

    def prepare(offset):
        block = wrap(y + offset, NY)
        values = L[block, :, 0:features].astype(F32)
        norms = split_rows_dot(ones, values * values, 2)
        BIAS[...] = KEEP[block] - scale * norms[0:1, :]

    def multiply(offset, who, part):
        block = wrap(y + offset, NY)
        at = part * 384 if isinstance(part, int) else pl.multiple_of(part * 384, 384)
        docs = D[who, pl.ds(at, 384), :]
        products = rows_dot(docs, L[block, :, 0:features])
        shift = DC[who, pl.ds(at, 384), :]
        shift = jnp.concatenate([shift, shift], axis=1)
        bias = jnp.concatenate(
            [jnp.broadcast_to(BIAS[pl.ds(who * 8 + part * 3 + i, 1), :], (128, 256)) for i in range(3)], axis=0
        )
        weights = jnp.exp2(products * (2.0 * scale) + shift + bias)
        groups = pl.ds(part * 8, 8)
        DG[who, groups] += (weights[:, 0:128] + weights[:, 128:256]).reshape(8, 48, 128)
        total = jnp.dot(weights.astype(BF16), L[block, :, features:], preferred_element_type=F32)
        PR[who, groups] += total.reshape(8, 48, 256)

    def multiply_all(offset, who):
        block = wrap(y + offset, NY)
        products = rows_dot(D[who], L[block, :, 0:features])
        shift = jnp.concatenate([DC[who], DC[who]], axis=1)
        bias = jnp.concatenate(
            [jnp.broadcast_to(BIAS[who * 8 + i : who * 8 + i + 1, :], (128, 256)) for i in range(6)], axis=0
        )
        weights = jnp.exp2(products * (2.0 * scale) + shift + bias)
        DG[who] += (weights[:, 0:128] + weights[:, 128:256]).reshape(16, 48, 128)
        total = jnp.dot(weights.astype(BF16), L[block, :, features:], preferred_element_type=F32)
        PR[who] += total.reshape(16, 48, 256)

    def batch(offset):
        from_x(offset)
        prepare(offset)

        for who in (1, 0):
            multiply_all(offset, who)

    def tell(step):
        pl.semaphore_signal(word.at[0, step], inc=1, device_id=front, device_id_type=MESH)
        pl.semaphore_signal(word.at[1, step], inc=1, device_id=back, device_id_type=MESH)

    def heard(step):
        pl.semaphore_wait(word.at[0, step], 1)
        pl.semaphore_wait(word.at[1, step], 1)

    for step in range(1, 5):
        from_y("A", 1, step)
        if step < 4:
            along_y("A", 1, step + 1)
        along_x("A", -step)
        from_y("B", -1, step)
        if step < 4:
            along_y("B", -1, step + 1)
        along_x("B", step)
        batch(-(step - 1))
        if step > 1:
            heard(step - 2)
        tell(step - 1)
        if step < 4:
            from_y("B", 1, step)
            if step < 3:
                along_y("B", 1, step + 1)
            along_x("B", -step)
            from_y("A", -1, step)
            if step < 3:
                along_y("A", -1, step + 1)
            along_x("A", step)
        if step > 1:
            batch(step - 1)

    heard(3)

    mine = x * 2 + core
    label = label_ref[...]
    high = lax.div(label, 32)
    low = label - 32 * high
    two = lax.broadcasted_iota(jnp.int32, (16, 48), 0)
    coded = jnp.where(two == 0, jnp.broadcast_to(high, (16, 48)), jnp.broadcast_to(low, (16, 48)))
    LB[mine] = jnp.zeros((16, 128), BF16)
    LB[mine, :, 0:48] = coded.astype(F32).astype(BF16)
    group = [(d, c) for d in range(NX) for c in range(2) if (d, c) != (0, 0)]

    def member(d, c):
        return wrap(x + d, NX), core if c == 0 else other

    from_x(4)
    prepare(4)
    for index, (d, c) in enumerate(group):
        to_x, to_core = member(d, c)
        sends.start(LB.at[mine], LB.at[mine], l_sem.at[index], device(to_x, y, to_core, z))
    far_first = (1 - x_high, x_high)
    for turn, part in enumerate(far_first):
        groups = pl.ds(part * 8, 8)
        multiply(4, 1, part)
        sends.start(PR.at[1, groups], PIN.at[groups], core_sem.at[2 + turn], partner)
        sends.start(DG.at[1, groups], DIN.at[groups], core_sem.at[4 + turn], partner)
    for part in far_first:
        multiply(4, 0, part)

    ones = jnp.ones((8, 128), BF16)

    def degrees(at):
        return split_rows_dot(ones, DG[0, at] + DIN[at], 3)[0:1, :]

    for turn, part in enumerate(far_first):
        groups = pl.ds(part * 8, 8)
        arrived(PIN.at[groups], core_sem, 2 + turn, partner)
        arrived(DIN.at[groups], core_sem, 4 + turn, partner)
        for d in range(turn, NZ):
            to = part * 8 + wrap(z + d, NZ)
            owner = {"blk": blk, "col": to}
            SP[to] = (PR[0, to] + PIN[to]).astype(BF16)
            SD[to, :, 0:48] = degrees(to)
            sends.start(SP.at[to], RP.at[col], col_sem.at[turn * 8 + d], owner)
            sends.start(SD.at[to], RD.at[col], cold_sem.at[turn * 8 + d], owner)
    projection = PR[0, col] + PIN[col]
    degree = degrees(col)
    for turn, part in enumerate(far_first):
        for d in range(turn, NZ):
            frm = part * 8 + wrap(z - d, NZ)
            owner = {"blk": blk, "col": frm}
            arrived(RP.at[frm], col_sem, turn * 8 + d, owner)
            arrived(RD.at[frm], cold_sem, turn * 8 + d, owner)
            projection = projection + RP[frm].astype(F32)
            degree = degree + RD[frm, :, 0:48]
    embedding = projection * lax.rsqrt(diagonal(degree, 48))
    emb_ref[...] = embedding
    unit = embedding * lax.rsqrt(jnp.sum(embedding * embedding, axis=1, keepdims=True) + 1e-6)

    halves = (0,)
    for h in halves:
        G[h, mine] = unit.astype(BF16)
        for index, (d, c) in enumerate(group):
            to_x, to_core = member(d, c)
            sends.start(G.at[h, mine], G.at[h, mine], g_sem.at[h, index], device(to_x, y, to_core, z))
    for index, (d, c) in enumerate(group):
        frm_x, frm_core = member(-d, c)
        arrived(LB.at[frm_x * 2 + frm_core], l_sem, index, device(frm_x, y, frm_core, z))
    clusters = (lax.broadcasted_iota(jnp.int32, (128, 48), 0) + mine * 128).astype(F32)
    hot = []
    for source in range(8):
        code = LB[source, :, 0:48].astype(F32)
        which = code[0:1, :] * 32.0 + code[1:2, :]
        hot.append(jnp.where(clusters == which, 1.0, 0.0).astype(BF16))

    for h in halves:
        for index, (d, c) in enumerate(group):
            frm_x, frm_core = member(-d, c)
            arrived(G.at[h, frm_x * 2 + frm_core], g_sem.at[h], index, device(frm_x, y, frm_core, z))
        sums = jnp.zeros((128, 256), F32)
        for source in range(8):
            sums = sums + jnp.dot(hot[source], G[h, source], preferred_element_type=F32)
        SY[h] = sums.reshape(8, 16, 256)
        for d in range(1, NY):
            to = wrap(y + d, NY)
            sends.start(SY.at[h, to], RY.at[h, y], ry_sem.at[h, d], device(x, to, core, z))

    for h in halves:
        RY[h, y] = SY[h, y]
        for d in range(1, NY):
            frm = wrap(y - d, NY)
            arrived(RY.at[h, frm], ry_sem.at[h], d, device(x, frm, core, z))
        total = RY[h, 0]
        for source in range(1, NY):
            total = total + RY[h, source]
        RZ[h, z] = total
        for d in range(1, NZ):
            sends.start(RZ.at[h, z], RZ.at[h, z], rz_sem.at[h, d], device(x, y, core, wrap(z + d, NZ)))

    for h in halves:
        for d in range(1, NZ):
            frm = wrap(z - d, NZ)
            arrived(RZ.at[h, frm], rz_sem.at[h], d, device(x, y, core, frm))
        total = RZ[h, 0]
        for source in range(1, NZ):
            total = total + RZ[h, source]
        W[h, mine, y] = total.astype(BF16)
        for d in range(1, NY):
            sends.start(W.at[h, mine, y], W.at[h, mine, y], wy_sem.at[h, d], device(x, wrap(y + d, NY), core, z))
    for h in halves:
        for d in range(1, NY):
            frm = wrap(y - d, NY)
            arrived(W.at[h, mine, frm], wy_sem.at[h], d, device(x, frm, core, z))
        for d in range(1, NX):
            sends.start(W.at[h, mine], W.at[h, mine], wx_sem.at[h, d], device(wrap(x + d, NX), y, core, z))
        sends.start(W.at[h, mine], W.at[h, mine], wc_sem.at[h, 0], partner)
    for h in halves:
        for d in range(1, NX):
            frm = wrap(x - d, NX)
            slot = frm * 2 + core
            arrived(W.at[h, slot], wx_sem.at[h], d, device(frm, y, core, z))
            sends.start(W.at[h, slot], W.at[h, slot], wc_sem.at[h, d], partner)
    for h in halves:
        for d in range(NX):
            frm = wrap(x - d, NX)
            arrived(W.at[h, frm * 2 + other], wc_sem.at[h], d, partner)
        cent_ref[...] = W[h].reshape(1024, 256)
    sends.finish()


def body(documents, landmarks, eigen_vectors, land_degree, eigen_values, tile_mask, labels):
    rows, features = documents.shape
    k = eigen_vectors.shape[1]
    dma = pltpu.SemaphoreType.DMA
    vmem = pl.BlockSpec(memory_space=pltpu.VMEM)
    embedding, centroids = pl.pallas_call(
        kernel,
        out_shape=(jax.ShapeDtypeStruct((48, k), F32), jax.ShapeDtypeStruct((1024, k), BF16)),
        in_specs=[pl.BlockSpec(memory_space=pl.ANY)] + [vmem] * 6,
        out_specs=(vmem, vmem),
        scratch_shapes=[
            pltpu.VMEM((NY, 4 * HALF, features + k), BF16),
            pltpu.VMEM((2, rows, features), BF16),
            pltpu.VMEM((2, rows, 128), F32),
            pltpu.VMEM((2, 8, 512), F32),
            pltpu.VMEM((NY, 16, 4 * HALF), F32),
            pltpu.VMEM((16, 4 * HALF), F32),
            pltpu.VMEM((2, 16, 48, k), F32),
            pltpu.VMEM((2, 16, 48, 128), F32),
            pltpu.VMEM((16, 48, k), F32),
            pltpu.VMEM((16, 48, 128), F32),
            pltpu.VMEM((16, 48, k), BF16),
            pltpu.VMEM((16, 48, k), BF16),
            pltpu.VMEM((16, 1, 128), F32),
            pltpu.VMEM((16, 1, 128), F32),
            pltpu.VMEM((8, 16, 128), BF16),
            pltpu.VMEM((1, 8, 48, 256), BF16),
            pltpu.VMEM((1, 8, 16, 256), F32),
            pltpu.VMEM((1, 8, 16, 256), F32),
            pltpu.VMEM((1, 8, 16, 256), F32),
            pltpu.VMEM((1, 8, 8, 16, 256), BF16),
            dma(()),
            dma((192,)),
            dma((4, 4)),
            dma((2, 8)),
            dma((8,)),
            dma((16,)),
            dma((16,)),
            dma((1, 8)),
            dma((1, 8)),
            dma((1, 8)),
            dma((1, 8)),
            dma((1, 4)),
            dma((1, 4)),
            dma((8,)),
            pltpu.SemaphoreType.REGULAR((2, 4)),
        ],
        compiler_params=pltpu.CompilerParams(collective_id=0, has_side_effects=True),
        name="nystrom",
    )(
        documents, landmarks, eigen_vectors, land_degree[None, :], eigen_values[None, :], tile_mask, labels[None, :]
    )
    return embedding, centroids[:C].astype(F32)


def solution(mesh):
    placed = (
        P("blk", None),
        P(("blk", "col"), None),
        P(("blk", "col"), None),
        P(("blk", "col")),
        P(),
        P("blk", None),
        P(("blk", "col")),
    )
    return jax.shard_map(
        body, mesh=mesh, in_specs=placed, out_specs=(P(("blk", "col"), None), P()), check_vma=False
    )
```

```python
import math
import jax
import jax.numpy as jnp
from jax import lax
from jax.experimental import pallas as pl
from jax.experimental.pallas import tpu as pltpu
from jax.sharding import PartitionSpec as P

C = 1000
BLOCK = 128
MESH = pl.DeviceIdType.MESH
F32, BF16 = jnp.float32, jnp.bfloat16
NX, NY, NZ = 4, 8, 8
FAR_FIRST = (4, 3, 5, 2, 6, 1, 7)
HALF = 64
DEAD = -1e30


def wrap(value, n):
    return lax.rem(value + n, n)


def device(x, y, core, z):
    x_high = lax.div(x, 2)
    x_low = x - 2 * x_high
    return {"blk": x_low * 16 + y * 2 + core, "col": x_high * 8 + z}


def rows_dot(a, b):
    return lax.dot_general(a, b, (((1,), (1,)), ((), ())), preferred_element_type=F32)


def split_rows_dot(ones, value, pieces):
    total, left = None, value
    for piece in range(pieces):
        part = left.astype(BF16)
        left = left - part.astype(F32)
        term = rows_dot(ones, part)
        total = term if total is None else total + term
    return total


def diagonal(row, n):
    square = jnp.broadcast_to(row, (n, n))
    down = lax.broadcasted_iota(jnp.int32, (n, n), 0)
    across = lax.broadcasted_iota(jnp.int32, (n, n), 1)
    return jnp.sum(jnp.where(down == across, square, 0.0), axis=1, keepdims=True)


class Sends:
    def __init__(self, sems):
        self.sems, self.used, self.open = sems, 0, []

    def start(self, src, dst, recv, to):
        copy = pltpu.make_async_remote_copy(
            src_ref=src, dst_ref=dst, send_sem=self.sems.at[self.used], recv_sem=recv,
            device_id=to, device_id_type=MESH,
        )
        self.used += 1
        copy.start()
        self.open.append(copy)

    def finish(self):
        for copy in self.open:
            copy.wait_send()


def arrived(ref, sems, index, frm):
    pltpu.make_async_remote_copy(
        src_ref=ref, dst_ref=ref, send_sem=sems.at[index], recv_sem=sems.at[index],
        device_id=frm, device_id_type=MESH,
    ).wait_recv()


def kernel(
    docs_ref, land_ref, vec_ref, ldeg_ref, eval_ref, mask_ref, label_ref,
    emb_ref, cent_ref,
    L, D, DC, M, KEEP, BIAS, PR, DG, PIN, DIN, SP, RP, SD, RD, LB, G, SY, RY, RZ, W,
    local_sem, send_sem, y_sem, x_sem, core_sem, col_sem, cold_sem, g_sem, ry_sem, rz_sem, wy_sem, wx_sem, wc_sem, l_sem, word, last_sem,
):
    blk, col = lax.axis_index("blk"), lax.axis_index("col")
    x_low = lax.div(blk, 16)
    core = lax.rem(blk, 2)
    y = lax.rem(lax.div(blk, 2), 8)
    x_high = lax.div(col, 8)
    z = lax.rem(col, 8)
    x = x_high * 2 + x_low
    other = 1 - core
    features = docs_ref.shape[1]
    scale = 4.0 / features * math.log2(math.e)

    partner = device(x, y, other, z)
    up, down = device(x, wrap(y + 1, NY), core, z), device(x, wrap(y - 1, NY), core, z)
    right, left = device(wrap(x + 1, NX), y, core, z), device(wrap(x - 1, NX), y, core, z)

    own_docs = pltpu.make_async_copy(docs_ref, D.at[0], local_sem)
    own_docs.start()

    barrier = pltpu.get_barrier_semaphore()
    front, back = device(x, y, core, wrap(z + 1, NZ)), device(x, y, core, wrap(z - 1, NZ))
    near = [partner, up, down, right, left, front, back]
    for peer in near:
        pl.semaphore_signal(barrier, inc=1, device_id=peer, device_id_type=MESH)

    inverse_root = diagonal(lax.rsqrt(ldeg_ref[...]), BLOCK)
    scaled = vec_ref[...].astype(F32) * inverse_root / eval_ref[...]
    L[y, 0:BLOCK, 0:features] = land_ref[...]
    L[y, 0:BLOCK, features:] = scaled.astype(BF16)
    M[0] = jnp.zeros(M.shape[1:], F32)
    M[0, 0:6, :] = mask_ref[...].astype(F32)
    pl.semaphore_wait(barrier, len(near))

    sends = Sends(send_sem)
    A, B = pl.ds(0, HALF), pl.ds(HALF, HALF)
    KINDS = {("A", 1): 0, ("B", 1): 1, ("A", -1): 2, ("B", -1): 3}

    def along_y(half, way, step):
        block = wrap(y - way * (step - 1), NY)
        piece = L.at[block, A if half == "A" else B]
        sends.start(piece, piece, y_sem.at[KINDS[half, way], step - 1], up if way == 1 else down)

    def along_x(half, offset):
        block = wrap(y + offset, NY)
        if half == "A":
            sends.start(L.at[block, A], L.at[block, pl.ds(2 * HALF, HALF)], x_sem.at[0, offset % NY], right)
        else:
            sends.start(L.at[block, B], L.at[block, pl.ds(3 * HALF, HALF)], x_sem.at[1, offset % NY], left)

    def from_y(half, way, step):
        block = wrap(y - way * step, NY)
        piece = L.at[block, A if half == "A" else B]
        arrived(piece, y_sem.at[KINDS[half, way]], step - 1, down if way == 1 else up)

    def from_x(offset):
        block = wrap(y + offset, NY)
        arrived(L.at[block, pl.ds(2 * HALF, HALF)], x_sem.at[0], offset % NY, left)
        arrived(L.at[block, pl.ds(3 * HALF, HALF)], x_sem.at[1], offset % NY, right)

    along_y("A", 1, 1)
    along_y("B", -1, 1)
    along_x("A", 0)
    along_x("B", 0)
    along_y("B", 1, 1)
    along_y("A", -1, 1)
    sends.start(M.at[0], M.at[1], core_sem.at[0], partner)
    own_docs.wait()
    sends.start(D.at[0], D.at[1], core_sem.at[1], partner)

    PR[...] = jnp.zeros(PR.shape, F32)
    DG[...] = jnp.zeros(DG.shape, F32)
    arrived(M.at[1], core_sem, 0, partner)
    live = M[...].reshape(16, M.shape[2])
    tiles = lax.broadcasted_iota(jnp.int32, live.shape, 1)
    segment = lax.div(lax.broadcasted_iota(jnp.int32, (16, 4 * HALF), 1), HALF)

    def tile_of(source_x, block):
        high = lax.div(source_x, 2)
        return (source_x - 2 * high) * 256 + block * 32 + core * 16 + high * 8 + z

    for block in range(NY):
        cols = [
            jnp.sum(jnp.where(tiles == tile_of(source, block), live, 0.0), axis=1, keepdims=True)
            for source in (x, wrap(x - 1, NX), wrap(x + 1, NX))
        ]
        keep = jnp.where(segment < 2, cols[0], jnp.where(segment < 3, cols[1], cols[2]))
        KEEP[block] = jnp.where(keep > 0.0, 0.0, DEAD)

    arrived(D.at[1], core_sem, 1, partner)

    def squares(chunk, carry):
        who, at = lax.div(chunk, 2), lax.rem(chunk, 2) * 384
        rows = D[who, pl.ds(pl.multiple_of(at, 384), 384), :].astype(F32)
        total = jnp.sum(rows * rows, axis=1, keepdims=True) * (-scale)
        DC[who, pl.ds(pl.multiple_of(at, 384), 384), :] = jnp.broadcast_to(total, (384, 128))
        return carry

    lax.fori_loop(0, 4, squares, 0)
    ones = jnp.ones((8, features), BF16)

    def prepare(offset):
        block = wrap(y + offset, NY)
        values = L[block, :, 0:features].astype(F32)
        norms = split_rows_dot(ones, values * values, 2)
        BIAS[...] = KEEP[block] - scale * norms[0:1, :]

    def multiply(offset, who, part):
        block = wrap(y + offset, NY)
        at = part * 384 if isinstance(part, int) else pl.multiple_of(part * 384, 384)
        docs = D[who, pl.ds(at, 384), :]
        products = rows_dot(docs, L[block, :, 0:features])
        shift = DC[who, pl.ds(at, 384), :]
        shift = jnp.concatenate([shift, shift], axis=1)
        bias = jnp.concatenate(
            [jnp.broadcast_to(BIAS[pl.ds(who * 8 + part * 3 + i, 1), :], (128, 256)) for i in range(3)], axis=0
        )
        weights = jnp.exp2(products * (2.0 * scale) + shift + bias)
        groups = pl.ds(part * 8, 8)
        DG[who, groups] += (weights[:, 0:128] + weights[:, 128:256]).reshape(8, 48, 128)
        total = jnp.dot(weights.astype(BF16), L[block, :, features:], preferred_element_type=F32)
        PR[who, groups] += total.reshape(8, 48, 256)

    def multiply_all(offset, who):
        block = wrap(y + offset, NY)
        products = rows_dot(D[who], L[block, :, 0:features])
        shift = jnp.concatenate([DC[who], DC[who]], axis=1)
        bias = jnp.concatenate(
            [jnp.broadcast_to(BIAS[who * 8 + i : who * 8 + i + 1, :], (128, 256)) for i in range(6)], axis=0
        )
        weights = jnp.exp2(products * (2.0 * scale) + shift + bias)
        DG[who] += (weights[:, 0:128] + weights[:, 128:256]).reshape(16, 48, 128)
        total = jnp.dot(weights.astype(BF16), L[block, :, features:], preferred_element_type=F32)
        PR[who] += total.reshape(16, 48, 256)

    def batch(offset):
        from_x(offset)
        prepare(offset)

        for who in (1, 0):
            multiply_all(offset, who)

    def tell(step):
        pl.semaphore_signal(word.at[0, step], inc=1, device_id=front, device_id_type=MESH)
        pl.semaphore_signal(word.at[1, step], inc=1, device_id=back, device_id_type=MESH)

    def heard(step):
        pl.semaphore_wait(word.at[0, step], 1)
        pl.semaphore_wait(word.at[1, step], 1)

    last = wrap(y + 4, NY)
    nearly = wrap(y - 3, NY), wrap(y + 3, NY)

    def last_along_y():
        for piece in (0, 1):
            a = L.at[nearly[0], pl.ds(piece * 32, 32)]
            sends.start(a, a, last_sem.at[0, piece], up)
            b = L.at[nearly[1], pl.ds(HALF + piece * 32, 32)]
            sends.start(b, b, last_sem.at[1, piece], down)

    def last_along_x():
        for piece in (0, 1):
            a = L.at[last, pl.ds(piece * 32, 32)]
            arrived(a, last_sem.at[0], piece, down)
            sends.start(a, L.at[last, pl.ds(2 * HALF + piece * 32, 32)], last_sem.at[2, piece], right)
            b = L.at[last, pl.ds(HALF + piece * 32, 32)]
            arrived(b, last_sem.at[1], piece, up)
            sends.start(b, L.at[last, pl.ds(3 * HALF + piece * 32, 32)], last_sem.at[3, piece], left)

    def last_from_x():
        for piece in (0, 1):
            arrived(L.at[last, pl.ds(2 * HALF + piece * 32, 32)], last_sem.at[2], piece, left)
            arrived(L.at[last, pl.ds(3 * HALF + piece * 32, 32)], last_sem.at[3], piece, right)

    for step in range(1, 5):
        if step == 4:
            last_along_x()
        else:
            from_y("A", 1, step)
            if step < 3:
                along_y("A", 1, step + 1)
            along_x("A", -step)
            from_y("B", -1, step)
            if step < 3:
                along_y("B", -1, step + 1)
            else:
                last_along_y()
            along_x("B", step)
        batch(-(step - 1))
        if step > 1:
            heard(step - 2)
        tell(step - 1)
        if step < 4:
            from_y("B", 1, step)
            if step < 3:
                along_y("B", 1, step + 1)
            along_x("B", -step)
            from_y("A", -1, step)
            if step < 3:
                along_y("A", -1, step + 1)
            along_x("A", step)
        if step > 1:
            batch(step - 1)

    heard(3)

    mine = x * 2 + core
    label = label_ref[...]
    high = lax.div(label, 32)
    low = label - 32 * high
    two = lax.broadcasted_iota(jnp.int32, (16, 48), 0)
    coded = jnp.where(two == 0, jnp.broadcast_to(high, (16, 48)), jnp.broadcast_to(low, (16, 48)))
    LB[mine] = jnp.zeros((16, 128), BF16)
    LB[mine, :, 0:48] = coded.astype(F32).astype(BF16)
    group = [(d, c) for d in range(NX) for c in range(2) if (d, c) != (0, 0)]

    def member(d, c):
        return wrap(x + d, NX), core if c == 0 else other

    last_from_x()
    prepare(4)
    for index, (d, c) in enumerate(group):
        to_x, to_core = member(d, c)
        sends.start(LB.at[mine], LB.at[mine], l_sem.at[index], device(to_x, y, to_core, z))
    far_first = (1 - x_high, x_high)
    for turn, part in enumerate(far_first):
        groups = pl.ds(part * 8, 8)
        multiply(4, 1, part)
        sends.start(PR.at[1, groups], PIN.at[groups], core_sem.at[2 + turn], partner)
        sends.start(DG.at[1, groups], DIN.at[groups], core_sem.at[4 + turn], partner)
    for part in far_first:
        multiply(4, 0, part)

    ones = jnp.ones((8, 128), BF16)

    def degrees(at):
        return split_rows_dot(ones, DG[0, at] + DIN[at], 3)[0:1, :]

    for turn, part in enumerate(far_first):
        groups = pl.ds(part * 8, 8)
        arrived(PIN.at[groups], core_sem, 2 + turn, partner)
        arrived(DIN.at[groups], core_sem, 4 + turn, partner)
        for d in FAR_FIRST + (0,) * (1 - turn):
            to = part * 8 + wrap(z + d, NZ)
            owner = {"blk": blk, "col": to}
            SP[to] = (PR[0, to] + PIN[to]).astype(BF16)
            SD[to, :, 0:48] = degrees(to)
            sends.start(SP.at[to], RP.at[col], col_sem.at[turn * 8 + d], owner)
            sends.start(SD.at[to], RD.at[col], cold_sem.at[turn * 8 + d], owner)
    projection = PR[0, col] + PIN[col]
    degree = degrees(col)
    for turn, part in enumerate(far_first):
        for d in range(turn, NZ):
            frm = part * 8 + wrap(z - d, NZ)
            owner = {"blk": blk, "col": frm}
            arrived(RP.at[frm], col_sem, turn * 8 + d, owner)
            arrived(RD.at[frm], cold_sem, turn * 8 + d, owner)
            projection = projection + RP[frm].astype(F32)
            degree = degree + RD[frm, :, 0:48]
    embedding = projection * lax.rsqrt(diagonal(degree, 48))
    emb_ref[...] = embedding
    unit = embedding * lax.rsqrt(jnp.sum(embedding * embedding, axis=1, keepdims=True) + 1e-6)

    halves = (0,)
    for h in halves:
        G[h, mine] = unit.astype(BF16)
        for index, (d, c) in enumerate(group):
            to_x, to_core = member(d, c)
            sends.start(G.at[h, mine], G.at[h, mine], g_sem.at[h, index], device(to_x, y, to_core, z))
    for index, (d, c) in enumerate(group):
        frm_x, frm_core = member(-d, c)
        arrived(LB.at[frm_x * 2 + frm_core], l_sem, index, device(frm_x, y, frm_core, z))
    clusters = (lax.broadcasted_iota(jnp.int32, (128, 48), 0) + mine * 128).astype(F32)
    hot = []
    for source in range(8):
        code = LB[source, :, 0:48].astype(F32)
        which = code[0:1, :] * 32.0 + code[1:2, :]
        hot.append(jnp.where(clusters == which, 1.0, 0.0).astype(BF16))

    for h in halves:
        for index, (d, c) in enumerate(group):
            frm_x, frm_core = member(-d, c)
            arrived(G.at[h, frm_x * 2 + frm_core], g_sem.at[h], index, device(frm_x, y, frm_core, z))
        sums = jnp.zeros((128, 256), F32)
        for source in range(8):
            sums = sums + jnp.dot(hot[source], G[h, source], preferred_element_type=F32)
        SY[h] = sums.reshape(8, 16, 256).astype(BF16)
        for d in FAR_FIRST:
            to = wrap(y + d, NY)
            sends.start(SY.at[h, to], RY.at[h, y], ry_sem.at[h, d], device(x, to, core, z))

    for h in halves:
        RY[h, y] = SY[h, y]
        for d in range(1, NY):
            frm = wrap(y - d, NY)
            arrived(RY.at[h, frm], ry_sem.at[h], d, device(x, frm, core, z))
        total = RY[h, 0].astype(F32)
        for source in range(1, NY):
            total = total + RY[h, source].astype(F32)
        RZ[h, z] = total.astype(BF16)
        for d in FAR_FIRST:
            sends.start(RZ.at[h, z], RZ.at[h, z], rz_sem.at[h, d], device(x, y, core, wrap(z + d, NZ)))

    for h in halves:
        for d in range(1, NZ):
            frm = wrap(z - d, NZ)
            arrived(RZ.at[h, frm], rz_sem.at[h], d, device(x, y, core, frm))
        total = RZ[h, 0].astype(F32)
        for source in range(1, NZ):
            total = total + RZ[h, source].astype(F32)
        W[h, mine, y] = total.astype(BF16)
        for d in FAR_FIRST:
            sends.start(W.at[h, mine, y], W.at[h, mine, y], wy_sem.at[h, d], device(x, wrap(y + d, NY), core, z))
    for h in halves:
        for d in range(1, NY):
            frm = wrap(y - d, NY)
            arrived(W.at[h, mine, frm], wy_sem.at[h], d, device(x, frm, core, z))
        for d in range(1, NX):
            sends.start(W.at[h, mine], W.at[h, mine], wx_sem.at[h, d], device(wrap(x + d, NX), y, core, z))
        sends.start(W.at[h, mine], W.at[h, mine], wc_sem.at[h, 0], partner)
    for h in halves:
        for d in range(1, NX):
            frm = wrap(x - d, NX)
            slot = frm * 2 + core
            arrived(W.at[h, slot], wx_sem.at[h], d, device(frm, y, core, z))
            sends.start(W.at[h, slot], W.at[h, slot], wc_sem.at[h, d], partner)
    for h in halves:
        for d in range(NX):
            frm = wrap(x - d, NX)
            arrived(W.at[h, frm * 2 + other], wc_sem.at[h], d, partner)
        cent_ref[...] = W[h].reshape(1024, 256)
    sends.finish()


def body(documents, landmarks, eigen_vectors, land_degree, eigen_values, tile_mask, labels):
    rows, features = documents.shape
    k = eigen_vectors.shape[1]
    dma = pltpu.SemaphoreType.DMA
    vmem = pl.BlockSpec(memory_space=pltpu.VMEM)
    embedding, centroids = pl.pallas_call(
        kernel,
        out_shape=(jax.ShapeDtypeStruct((48, k), F32), jax.ShapeDtypeStruct((1024, k), BF16)),
        in_specs=[pl.BlockSpec(memory_space=pl.ANY)] + [vmem] * 6,
        out_specs=(vmem, vmem),
        scratch_shapes=[
            pltpu.VMEM((NY, 4 * HALF, features + k), BF16),
            pltpu.VMEM((2, rows, features), BF16),
            pltpu.VMEM((2, rows, 128), F32),
            pltpu.VMEM((2, 8, 512), F32),
            pltpu.VMEM((NY, 16, 4 * HALF), F32),
            pltpu.VMEM((16, 4 * HALF), F32),
            pltpu.VMEM((2, 16, 48, k), F32),
            pltpu.VMEM((2, 16, 48, 128), F32),
            pltpu.VMEM((16, 48, k), F32),
            pltpu.VMEM((16, 48, 128), F32),
            pltpu.VMEM((16, 48, k), BF16),
            pltpu.VMEM((16, 48, k), BF16),
            pltpu.VMEM((16, 1, 128), F32),
            pltpu.VMEM((16, 1, 128), F32),
            pltpu.VMEM((8, 16, 128), BF16),
            pltpu.VMEM((1, 8, 48, 256), BF16),
            pltpu.VMEM((1, 8, 16, 256), BF16),
            pltpu.VMEM((1, 8, 16, 256), BF16),
            pltpu.VMEM((1, 8, 16, 256), BF16),
            pltpu.VMEM((1, 8, 8, 16, 256), BF16),
            dma(()),
            dma((192,)),
            dma((4, 4)),
            dma((2, 8)),
            dma((8,)),
            dma((16,)),
            dma((16,)),
            dma((1, 8)),
            dma((1, 8)),
            dma((1, 8)),
            dma((1, 8)),
            dma((1, 4)),
            dma((1, 4)),
            dma((8,)),
            pltpu.SemaphoreType.REGULAR((2, 4)),
            dma((4, 2)),
        ],
        compiler_params=pltpu.CompilerParams(collective_id=0, has_side_effects=True),
        name="nystrom",
    )(
        documents, landmarks, eigen_vectors, land_degree[None, :], eigen_values[None, :], tile_mask, labels[None, :]
    )
    return embedding, centroids[:C].astype(F32)


def solution(mesh):
    placed = (
        P("blk", None),
        P(("blk", "col"), None),
        P(("blk", "col"), None),
        P(("blk", "col")),
        P(),
        P("blk", None),
        P(("blk", "col")),
    )
    return jax.shard_map(
        body, mesh=mesh, in_specs=placed, out_specs=(P(("blk", "col"), None), P()), check_vma=False
    )
```
